32 devices in a mesh: tm: 16 (over z, y, x), batch: 2 (over core).
Axes of the slice: x: 2, y: 2, z: 4, core: 2. Of those that a mesh axis runs over, the one named last changes fastest.
Arguments:
- state_map: float32 [512, 256, 256], P(('batch', 'tm')), parts along dimension 0, may hold values from -0.375 to 0.375
- input_map: float32 [512, 64, 256], P(('batch', 'tm')), parts along dimension 0, may hold values from -0.375 to 0.375
- closed_loop: float32 [512, 256, 256], P(('batch', 'tm')), parts along dimension 0, may hold values from -1.001 to 1.001
- feedback: float32 [512, 64, 256], P(('batch', 'tm')), parts along dimension 0, may hold values from -0.375 to 0.375
- value_matrix: float32 [512, 256, 256], P(('batch', 'tm')), parts along dimension 0, may hold values from -0.046875 to 1.5, as said below
- gain_inverse: float32 [512, 64, 64], P(('batch', 'tm')), parts along dimension 0, may hold values from -0.0105 to 0.2, as said below
- input_weight: float32 [128, 64], P('batch'), parts along dimension 0, may hold values from -0.36 to 6, as said below
- state_weight: float32 [512, 256], P(('batch', 'tm')), parts along dimension 0, may hold values from 0.1 to 3
- state_linear: float32 [512, 256], P(('batch', 'tm')), parts along dimension 0, may hold values from -0.18 to 0.18
- input_linear: float32 [512, 64], P(('batch', 'tm')), parts along dimension 0, may hold values from -0.18 to 0.18
- offset: float32 [512, 256], P(('batch', 'tm')), parts along dimension 0, may hold values from -0.18 to 0.18
- upper_bound: float32 [512, 64], P(('batch', 'tm')), parts along dimension 0, may hold values from 0.1 to 0.3
- states: float32 [512, 256], P(('batch', 'tm')), parts along dimension 0, may hold values from -0.18 to 0.18
- inputs: float32 [512, 64], P(('batch', 'tm')), parts along dimension 0, may hold values from -0.18 to 0.18
- multipliers: float32 [512, 256], P(('batch', 'tm')), parts along dimension 0, may hold values from -0.18 to 0.18
- bound_mult: float32 [512, 64], P(('batch', 'tm')), parts along dimension 0, may hold values from 0 to 0.06
- active: int32 [512, 64], P(('batch', 'tm')), parts along dimension 0, may hold values 0 or 1
Outputs:
- state_step: float32 [512, 256], P(('batch', 'tm')), parts along dimension 0
- input_step: float32 [512, 64], P(('batch', 'tm')), parts along dimension 0
- multiplier_step: float32 [512, 256], P(('batch', 'tm')), parts along dimension 0
- bound_step: float32 [512, 64], P(('batch', 'tm')), parts along dimension 0
- kkt_norms: float32 [6], P('batch'), parts along dimension 0
The draws below stay inside these ranges and needn't reach their ends.
There are 2 independent parts, one for each index of `batch`. The reference program is written for one: setup_inputs(seed, part) draws one part's arguments, and reference() takes and returns one part's arrays. A program takes and returns all parts, laid end to end along the dimension named above; each array names one. Nothing has to cross between parts.
Inputs may be any that keep to these rules, and one draw needn't show every extreme that they name: `value_matrix`: each section's matrix is symmetric. `gain_inverse`: each section's matrix is symmetric. `input_weight`: symmetric.
All inputs are finite; a program needn't handle non-finite values. No bound on the sum of `active` on one device may be relied on, other than what follows from the above.
Results may differ from the reference program's by a relative error of at most 0.0003.
Values sent between devices are 32-bit elements; how exact they have to be, the bound alone decides.
A program may use at most 128 MiB of HBM per device.

```python
import math
import jax
import jax.numpy as jnp
from jax import lax

NS = 256
NU = 64
HORIZON = 256


def symmetric_draw(key, sections, dimension, lowest, highest, spread):
    first_key, second_key = jax.random.split(key)
    diagonal = jax.random.uniform(first_key, (sections, dimension), jnp.float32, lowest, highest)
    noise_raw = jax.random.normal(second_key, (sections, dimension, dimension), jnp.float32) * spread
    mixed = jnp.clip((noise_raw + jnp.swapaxes(noise_raw, 1, 2)) / math.sqrt(2.0), -3.0 * spread, 3.0 * spread)
    identity = jnp.eye(dimension, dtype=jnp.float32)
    return mixed * (1.0 - identity) + diagonal[:, :, None] * identity


def draw_value_matrix(key, part):
    return symmetric_draw(jax.random.fold_in(key, 11), HORIZON, NS, 0.5, 1.5, 0.25 / math.sqrt(NS))


def draw_gain_inverse(key, part):
    return symmetric_draw(jax.random.fold_in(key, 12), HORIZON, NU, 0.08, 0.2, 0.028 / math.sqrt(NU))


def draw_input_weight(key, part):
    return symmetric_draw(jax.random.fold_in(key, 13), 1, NU, 2.0, 6.0, 0.96 / math.sqrt(NU))[0]


def draw_closed_loop(key, part):
    subkeys = jax.random.split(jax.random.fold_in(key, 7), 5)
    ranking = jax.random.permutation(subkeys[0], NS)
    slow_total = NS // 2
    slow_channel = ranking < slow_total
    same_class = (slow_channel[:, None] == slow_channel[None, :]).astype(jnp.float32)
    slow_rate = jax.random.uniform(subkeys[1], (HORIZON, NS), jnp.float32, 0.3, 2.0) / HORIZON
    memory = jnp.exp(jax.random.uniform(subkeys[2], (HORIZON, NS), jnp.float32, math.log(2.0), math.log(8.0)))
    decays = jnp.where(slow_channel[None, :], jnp.exp(-slow_rate), jnp.exp(-1.0 / memory))
    noise_raw = jax.random.normal(subkeys[3], (HORIZON, NS, NS), jnp.float32) * (0.5 / math.sqrt(NS))
    cross_raw = jax.random.normal(subkeys[4], (HORIZON, NS, NS), jnp.float32) * (0.25 / math.sqrt(NS * HORIZON))
    within_part = (noise_raw - jnp.swapaxes(noise_raw, 1, 2)) * same_class
    between_part = (cross_raw - jnp.swapaxes(cross_raw, 1, 2)) * (1.0 - same_class)
    skew_part = within_part + between_part
    identity = jnp.eye(NS, dtype=jnp.float32)
    rotation = jnp.linalg.solve(identity + skew_part, identity - skew_part)
    return decays[:, :, None] * rotation


def with_ends(array, stream_key, low, top_value):
    spot = [jax.random.randint(jax.random.fold_in(stream_key, axis), (), 0, length) for axis, length in enumerate(array.shape)]
    main_axis = array.shape.index(max(array.shape))
    next_to = spot[:main_axis] + [(spot[main_axis] + 1) % array.shape[main_axis]] + spot[main_axis + 1:]
    return array.at[tuple(spot)].set(low).at[tuple(next_to)].set(top_value)


def block_scale(key, dims, shards, low, high):
    level = 1.0
    for axis_at, blocks in shards:
        draws = jax.random.uniform(jax.random.fold_in(jax.random.fold_in(key, 6), axis_at), (blocks,), jnp.float32, low / len(shards), high / len(shards))
        level = level * jnp.repeat(jnp.exp(draws), dims[axis_at] // blocks).reshape((-1,) + (1,) * (len(dims) - 1 - axis_at))
    return level


def noise(own_key, shape, scale, limit, cuts=(), kind=jnp.bfloat16):
    drawn = jax.random.normal(own_key, shape, jnp.float32) * scale
    if len(cuts) > 0:
        drawn = block_scale(own_key, shape, cuts, -0.22, 0.18) * drawn
    return jnp.clip(drawn, min=-limit, max=limit).astype(kind)


def setup_inputs(seed: int = 0, part: int = 0) -> dict:
    key_list = jax.random.split(jax.random.key(seed), 18)
    part_splits = jax.random.split(jax.random.fold_in(key_list[17], part), 18)
    state_map = noise(part_splits[0], (HORIZON, NS, NS), NS ** -0.5, 0.375, ((0, 16),), jnp.float32)
    input_map = noise(part_splits[1], (HORIZON, NU, NS), NS ** -0.5, 0.375, ((0, 16),), jnp.float32)
    closed_loop = draw_closed_loop(jax.random.fold_in(jax.random.fold_in(key_list[17], part), 71), part)
    feedback = noise(part_splits[3], (HORIZON, NU, NS), NS ** -0.5, 0.375, ((0, 16),), jnp.float32)
    value_matrix = draw_value_matrix(jax.random.fold_in(jax.random.fold_in(key_list[17], part), 71), part)
    gain_inverse = draw_gain_inverse(jax.random.fold_in(jax.random.fold_in(key_list[17], part), 71), part)
    input_weight = draw_input_weight(jax.random.fold_in(jax.random.fold_in(key_list[17], part), 71), part)
    state_weight = jnp.clip(jnp.exp(math.log(3.0) - 3.4011974 * jax.random.uniform(part_splits[7], (HORIZON, NS), jnp.float32) ** block_scale(part_splits[7], (HORIZON, NS), ((0, 16),), -0.2, 0.2)), 0.1, 3.0)
    state_linear = noise(part_splits[8], (HORIZON, NS), 0.03, 0.18, ((0, 16),), jnp.float32)
    input_linear = noise(part_splits[9], (HORIZON, NU), 0.03, 0.18, ((0, 16),), jnp.float32)
    offset = noise(part_splits[10], (HORIZON, NS), 0.03, 0.18, ((0, 16),), jnp.float32)
    upper_bound = jnp.clip(0.1 + 0.20000001043081284 * jax.random.uniform(part_splits[11], (HORIZON, NU), jnp.float32) ** block_scale(part_splits[11], (HORIZON, NU), ((0, 16),), -0.2, 0.2), 0.1, 0.3)
    states = noise(part_splits[12], (HORIZON, NS), 0.03, 0.18, ((0, 16),), jnp.float32)
    inputs = noise(part_splits[13], (HORIZON, NU), 0.03, 0.18, ((0, 16),), jnp.float32)
    multipliers = noise(part_splits[14], (HORIZON, NS), 0.03, 0.18, ((0, 16),), jnp.float32)
    bound_mult = jnp.clip(0.06 * jax.random.uniform(part_splits[15], (HORIZON, NU), jnp.float32) ** block_scale(part_splits[15], (HORIZON, NU), ((0, 16),), -0.2, 0.2), 0.0, 0.06)
    active = with_ends((jax.random.randint(part_splits[16], (HORIZON, NU), 0, 3) < 1).astype(jnp.int32), jax.random.fold_in(part_splits[16], 1), 0, 1)
    return dict(state_map=state_map, input_map=input_map, closed_loop=closed_loop, feedback=feedback, value_matrix=value_matrix, gain_inverse=gain_inverse, input_weight=input_weight, state_weight=state_weight, state_linear=state_linear, input_linear=input_linear, offset=offset, upper_bound=upper_bound, states=states, inputs=inputs, multipliers=multipliers, bound_mult=bound_mult, active=active)


PRECISE = lax.Precision.HIGHEST
floor_share = 0.001

def apply_each(matrices, vectors):
    return jnp.einsum('kij,kj->ki', matrices, vectors, precision=PRECISE)

def apply_transposed(matrices, vectors):
    return jnp.einsum('kji,kj->ki', matrices, vectors, precision=PRECISE)

def backward_sweep(loop_mats, sources, incoming):

    def section(costate, section_item):
        matrix, source = section_item
        earlier = jnp.dot(costate, matrix, precision=PRECISE) + source
        return (earlier, (costate, earlier))
    final_state, (after, before) = lax.scan(section, incoming, (loop_mats, sources), reverse=True)
    return (after, before, final_state)

def forward_sweep(loop_mats, defects, pushes, entering):

    def section(carried, section_item):
        matrix, defect, pushed = section_item
        correction = carried - defect
        return (jnp.dot(matrix, correction, precision=PRECISE) + pushed, correction)
    final_state, steps = lax.scan(section, entering, (loop_mats, defects, pushes))
    return (steps, final_state)

def make_statistics(defect, grad_state, grad_input, slack_gap, offset, state_linear, input_linear, bound_mult):
    return jnp.stack([jnp.sum(defect * defect), jnp.sum(grad_state * grad_state) + jnp.sum(grad_input * grad_input), jnp.sum(slack_gap * slack_gap), jnp.sum(offset * offset), jnp.sum(state_linear * state_linear) + jnp.sum(input_linear * input_linear), jnp.sum(bound_mult * bound_mult)])

def make_norms(totals, horizon, state_count, input_count):
    primal = totals[0] / (totals[3] + floor_share * horizon * state_count)
    dual = totals[1] / (totals[4] + floor_share * horizon * (state_count + input_count))
    complement = totals[2] / (totals[5] + floor_share * horizon * input_count)
    return jnp.sqrt(jnp.stack([primal, dual, complement]))

def reference(state_map, input_map, closed_loop, feedback, value_matrix, gain_inverse, input_weight, state_weight, state_linear, input_linear, offset, upper_bound, states, inputs, multipliers, bound_mult, active):
    state_count = states.shape[1]
    input_count = inputs.shape[1]
    horizon = states.shape[0]
    predicted = apply_each(state_map, states) + apply_transposed(input_map, inputs)
    previous = jnp.concatenate([jnp.zeros((1, state_count), jnp.float32), predicted[:-1]], axis=0)
    defect = states - previous - offset
    following = jnp.concatenate([multipliers[1:], jnp.zeros((1, state_count), jnp.float32)], axis=0)
    grad_state = state_weight * states + state_linear + multipliers - apply_transposed(state_map, following)
    grad_input = jnp.einsum('ij,kj->ki', input_weight, inputs, precision=PRECISE) + input_linear - apply_each(input_map, following) + bound_mult
    slack_gap = bound_mult * (upper_bound - inputs)
    sources = apply_each(value_matrix, defect) + grad_state + apply_transposed(feedback, grad_input)
    after, before, unused = backward_sweep(closed_loop, sources, jnp.zeros((state_count,), jnp.float32))
    pulled = apply_each(input_map, after)
    forward_gain = -apply_each(gain_inverse, grad_input + pulled)
    pushes = apply_transposed(input_map, forward_gain)
    state_step, unused_final = forward_sweep(closed_loop, defect, pushes, jnp.zeros((state_count,), jnp.float32))
    chosen = active.astype(jnp.float32)
    input_step = (1.0 - chosen) * (apply_each(feedback, state_step) + forward_gain) + chosen * (upper_bound - inputs)
    multiplier_step = apply_each(value_matrix, state_step - defect) + before
    bound_step = chosen * (grad_input + jnp.einsum('ij,kj->ki', input_weight, input_step, precision=PRECISE) + pulled)
    totals = make_statistics(defect, grad_state, grad_input, slack_gap, offset, state_linear, input_linear, bound_mult)
    kkt_norms = make_norms(totals, horizon, state_count, input_count)
    return (state_step, input_step, multiplier_step, bound_step, kkt_norms)
```

```python
import functools
import jax
import jax.numpy as jnp
from jax import lax
from jax.experimental import pallas as pl
from jax.experimental.pallas import tpu as pltpu
from jax.sharding import PartitionSpec as P

F32 = jnp.float32
BF16 = jnp.bfloat16
PRECISE = lax.Precision.HIGHEST
MESH = pl.DeviceIdType.MESH
floor_share = 0.001
LANES = 128


def parts_of(x):
    high = x.astype(BF16)
    return high, (x - high.astype(F32)).astype(BF16)


def matmul(a, b):
    ah, al = parts_of(a)
    bh, bl = parts_of(b)
    dot = functools.partial(jnp.dot, preferred_element_type=F32)
    return dot(ah, bh) + (dot(ah, bl) + dot(al, bh))


def turned(x):
    rows, cols = x.shape
    up = -rows % LANES
    side = -cols % LANES
    if up:
        x = jnp.concatenate([x, jnp.zeros((up, cols), F32)], axis=0)
    if side:
        x = jnp.concatenate([x, jnp.zeros((rows + up, side), F32)], axis=1)
    return x.T[:cols, :rows]


def column(row):
    return jnp.broadcast_to(row, (LANES, row.shape[1])).T[:, :1]


def row_of(col):
    return jnp.broadcast_to(col, (col.shape[0], LANES)).T[:1]


def times(matrix, row):
    return jnp.sum(matrix * row, axis=1, keepdims=True)


def times_t(matrix, col):
    return jnp.sum(matrix * col, axis=0, keepdims=True)


def kernel(n, size, *refs):
    (a_hbm, b_hbm, m_hbm, k_hbm, v_hbm, gi_hbm, w_hbm, sw_hbm, sl_hbm, il_hbm, of_hbm, ub_hbm,
     st_hbm, in_hbm, mu_hbm, bm_hbm, ac_hbm,
     o_state, o_input, o_mult, o_bound, o_norm,
     a, b, m, fb, v, gi, w, sw, sl, il, of, ub, st, inp, mu, bm, ac,
     pre, suf, group, whole, sources, pushes, back_local, fwd_local, back,
     cols, fol_in, prd_in, prd_out, fol_out, vec_b, vec_f, ch_b_in, ch_f_in, ch_b_out, ch_f_out,
     load_sem, m_sem, nb_send, nb_recv, p_send, p_recv, b_send, b_recv, f_send, f_recv,
     ch_send, ch_recv) = refs
    me = lax.axis_index("tm")
    place = lax.rem(me, size)
    base = me - place
    at_group = lax.div(me, size)
    groups = n // size
    sections, ns = st.shape
    nu = inp.shape[1]
    half = sections // 2

    order = []
    for i in range(half):
        order += [i, sections - 1 - i]
    for k in order:
        pltpu.make_async_copy(m_hbm.at[k], m.at[k], m_sem.at[k]).start()
    small = [(w_hbm, w), (sw_hbm, sw), (sl_hbm, sl), (il_hbm, il), (of_hbm, of), (ub_hbm, ub),
             (st_hbm, st), (in_hbm, inp), (mu_hbm, mu), (bm_hbm, bm), (ac_hbm, ac)]
    large = [(a_hbm, a), (b_hbm, b), (v_hbm, v), (k_hbm, fb), (gi_hbm, gi)]
    loads = [
        pltpu.make_async_copy(src, dst, load_sem.at[i]) for i, (src, dst) in enumerate(small + large)
    ]
    for load in loads:
        load.start()

    barrier = pltpu.get_barrier_semaphore()
    first_of, last_of = place == 0, place == size - 1
    relations = [
        (jnp.logical_and(first_of, me > 0), me - 1),
        (jnp.logical_and(last_of, me < n - 1), me + 1),
        (at_group > 0, me - size),
        (at_group < groups - 1, me + size),
    ]
    mates = [base + lax.rem(place + j, size) for j in range(1, size)]
    for mate in mates:
        pl.semaphore_signal(barrier, inc=1, device_id={"tm": mate}, device_id_type=MESH)
    for holds, peer in relations:
        @pl.when(holds)
        def _():
            pl.semaphore_signal(barrier, inc=1, device_id={"tm": peer}, device_id_type=MESH)
    peers = size - 1
    for holds, peer in relations:
        peers = peers + jnp.where(holds, 1, 0)
    pl.semaphore_wait(barrier, peers)

    def remote(src, dst, send, recv, peer):
        return pltpu.make_async_remote_copy(
            src_ref=src, dst_ref=dst, send_sem=send, recv_sem=recv,
            device_id={"tm": peer}, device_id_type=MESH,
        )

    for load in loads[: len(small)]:
        load.wait()
    to_earlier = remote(fol_out, fol_in, nb_send.at[0], nb_recv.at[0], me - 1)
    to_later = remote(prd_out, prd_in, nb_send.at[1], nb_recv.at[1], me + 1)
    fol_out[...] = jnp.broadcast_to(mu[0:1], fol_out.shape)

    @pl.when(me > 0)
    def _():
        to_earlier.start()

    def wait_loop(k):
        pltpu.make_async_copy(m_hbm.at[k], m.at[k], m_sem.at[k]).wait()

    wait_loop(0)
    wait_loop(sections - 1)
    pre[0] = m[0]
    suf[sections - 1] = m[sections - 1]

    def grow(i, waits):
        j = sections - 1 - i
        if waits:
            wait_loop(i)
            wait_loop(j)
        pre[i] = matmul(m[i], pre[i - 1])
        suf[j] = matmul(suf[j + 1], m[j])

    @pl.loop(1, half)
    def _(i):
        grow(i, True)

    product = matmul(suf[half], pre[half - 1])
    suf[0] = product
    group[pl.ds(place, 1)] = product[None]
    p_copies = [
        remote(group.at[place], group.at[place], p_send.at[j], p_recv.at[j], mate)
        for j, mate in enumerate(mates)
    ]
    for copy in p_copies:
        copy.start()

    for load in loads[len(small):]:
        load.wait()
    lane = lax.broadcasted_iota(jnp.int32, (ns, LANES), 1)
    lane_u = lax.broadcasted_iota(jnp.int32, (nu, LANES), 1)

    inputs_t = turned(inp[...])
    acc = jnp.zeros((ns, LANES), F32)
    for k in range(sections):
        acc = jnp.where(lane == k, times(a[k], st[k:k + 1]), acc)
    predicted = acc.T[:sections]
    rows = [times_t(b[k], inputs_t[:, k:k + 1]) for k in range(sections)]
    predicted = predicted + jnp.concatenate(rows, axis=0)
    prd_out[...] = jnp.broadcast_to(predicted[sections - 1:], prd_out.shape)

    @pl.when(me < n - 1)
    def _():
        to_later.start()

    @pl.loop(half, sections - 1)
    def _(i):
        grow(i, False)

    @pl.when(me < n - 1)
    def _():
        to_earlier.wait_recv()

    @pl.when(me == n - 1)
    def _():
        fol_in[...] = jnp.zeros_like(fol_in)

    following = jnp.concatenate([mu[1:], fol_in[0:1]], axis=0)
    following_t = turned(following)
    grad_input = (
        jnp.dot(inp[...], w[...], precision=PRECISE, preferred_element_type=F32) + il[...] + bm[...]
    )
    acc = jnp.zeros((nu, LANES), F32)
    for k in range(sections):
        acc = jnp.where(lane_u == k, times(b[k], following[k:k + 1]), acc)
    grad_input = grad_input - turned(acc)[:sections]
    grad_input_t = turned(grad_input)
    rows = [times_t(a[k], following_t[:, k:k + 1]) for k in range(sections)]
    grad_state = sw[...] * st[...] + sl[...] + mu[...] - jnp.concatenate(rows, axis=0)

    @pl.when(me > 0)
    def _():
        to_later.wait_recv()

    @pl.when(me == 0)
    def _():
        prd_in[...] = jnp.zeros_like(prd_in)

    previous = jnp.concatenate([prd_in[0:1], predicted[:sections - 1]], axis=0)
    defect = st[...] - previous - of[...]
    defect_t = turned(defect)
    rows = [
        times_t(v[k], defect_t[:, k:k + 1]) + times_t(fb[k], grad_input_t[:, k:k + 1])
        for k in range(sections)
    ]
    sources[...] = jnp.concatenate(rows, axis=0) + grad_state
    slack = bm[...] * (ub[...] - inp[...])

    def total(*xs):
        return sum(
            jnp.sum(jnp.sum(x * x, axis=1, keepdims=True), axis=0, keepdims=True) for x in xs
        )

    sums = [total(defect), total(grad_state, grad_input), total(slack), total(of[...]),
            total(sl[...], il[...]), total(bm[...])]
    line = lax.broadcasted_iota(jnp.int32, (1, ns), 1)
    stats = jnp.zeros((1, ns), F32)
    for i, value in enumerate(sums):
        stats = jnp.where(line == i, value, stats)

    def packed(vector, extra):
        return jnp.concatenate([vector, extra, jnp.zeros((6, ns), F32)], axis=0)

    costate = sources[sections - 1:]
    back_local[sections - 1:] = costate
    for k in range(sections - 2, -1, -1):
        costate = times_t(m[k], column(costate)) + sources[k:k + 1]
        back_local[k:k + 1] = costate
    vec_b[pl.ds(place, 1)] = packed(costate, stats)[None]
    b_copies = [
        remote(vec_b.at[place], vec_b.at[place], b_send.at[j], b_recv.at[j], mate)
        for j, mate in enumerate(mates)
    ]
    for copy in b_copies:
        copy.start()

    def arrive(buffer, send, recv):
        for j in range(size - 1):
            source = base + lax.rem(place + size - 1 - j, size)
            slot = source - base
            remote(buffer.at[slot], buffer.at[slot], send.at[j], recv.at[j], source).wait_recv()

    arrive(vec_b, b_send, b_recv)
    arrive(group, p_send, p_recv)
    joined = group[0]
    for e in range(1, size):
        joined = matmul(group[e], joined)
    whole[...] = joined
    group_stats = jnp.sum(vec_b[:, 1, :], axis=0, keepdims=True)

    y = vec_b[size - 1, 0:1]
    for e in range(size - 2, -1, -1):
        y = vec_b[e, 0:1] + times_t(group[e], column(y))
    to_before = remote(ch_b_out, ch_b_in, ch_send.at[0], ch_recv.at[0], me - size)
    to_after = remote(ch_f_out, ch_f_in, ch_send.at[1], ch_recv.at[1], me + size)

    @pl.when(at_group < groups - 1)
    def _():
        to_before.wait_recv()

    @pl.when(at_group == groups - 1)
    def _():
        ch_b_in[...] = jnp.zeros_like(ch_b_in)

    incoming = ch_b_in[0:1]
    above = ch_b_in[1:2]
    ch_b_out[...] = packed(times_t(whole[...], column(incoming)) + y, above + group_stats)

    @pl.when(at_group > 0)
    def _():
        to_before.start()

    for e in range(size - 1, 0, -1):
        new = vec_b[e, 0:1] + times_t(group[e], column(incoming))
        incoming = jnp.where(place < e, new, incoming)

    incoming_c = column(incoming)
    for k in range(sections):
        back[k:k + 1] = times_t(suf[k], incoming_c) + back_local[k:k + 1]
    before = back[...]
    after = jnp.concatenate([before[1:], incoming], axis=0)
    acc = jnp.zeros((nu, LANES), F32)
    for k in range(sections):
        acc = jnp.where(lane_u == k, times(b[k], after[k:k + 1]), acc)
    pulled = turned(acc)[:sections]
    held = grad_input + pulled
    acc = jnp.zeros((nu, LANES), F32)
    for k in range(sections):
        gain = -times(gi[k], held[k:k + 1])
        acc = jnp.where(lane_u == k, gain, acc)
        pushes[k:k + 1] = times_t(b[k], gain)
    forward_gain = turned(acc)[:sections]

    acc = jnp.zeros((ns, ns), F32)
    for k in range(sections):
        drive = -defect[k:k + 1]
        if k:
            drive = drive + pushes[k - 1:k]
        acc = acc + suf[k] * drive
    ended = row_of(jnp.sum(acc, axis=1, keepdims=True)) + pushes[sections - 1:]
    vec_f[pl.ds(place, 1)] = packed(ended, stats)[None]
    f_copies = [
        remote(vec_f.at[place], vec_f.at[place], f_send.at[j], f_recv.at[j], mate)
        for j, mate in enumerate(mates)
    ]
    for copy in f_copies:
        copy.start()

    step = -defect[0:1]
    acc = jnp.where(lane == 0, column(step), 0.0)
    for k in range(1, sections):
        moved = times(m[k - 1], step)
        step = row_of(moved) + pushes[k - 1:k] - defect[k:k + 1]
        acc = jnp.where(lane == k, column(step), acc)
    cols[...] = acc

    arrive(vec_f, f_send, f_recv)
    y = vec_f[0, 0:1]
    for e in range(1, size):
        y = vec_f[e, 0:1] + row_of(times(group[e], y))

    @pl.when(at_group > 0)
    def _():
        to_after.wait_recv()

    @pl.when(at_group == 0)
    def _():
        ch_f_in[...] = jnp.zeros_like(ch_f_in)

    entering = ch_f_in[0:1]
    below = ch_f_in[1:2]
    ch_f_out[...] = packed(row_of(times(whole[...], entering)) + y, below + group_stats)

    @pl.when(at_group < groups - 1)
    def _():
        to_after.start()

    for e in range(size - 1):
        new = vec_f[e, 0:1] + row_of(times(group[e], entering))
        entering = jnp.where(place > e, new, entering)

    acc = cols[...] + jnp.where(lane == 0, column(entering), 0.0)
    for k in range(1, sections):
        acc = acc + jnp.where(lane == k, times(pre[k - 1], entering), 0.0)
    state_step = acc.T[:sections]
    o_state[...] = state_step
    moved = acc[:, :sections] - defect_t
    for k in range(sections):
        o_mult[k:k + 1] = times_t(v[k], moved[:, k:k + 1]) + back[k:k + 1]
    acc = jnp.zeros((nu, LANES), F32)
    for k in range(sections):
        acc = jnp.where(lane_u == k, times(fb[k], state_step[k:k + 1]), acc)
    fed = turned(acc)[:sections]
    chosen = ac[...].astype(F32)
    input_step = (1.0 - chosen) * (fed + forward_gain) + chosen * (ub[...] - inp[...])
    o_input[...] = input_step
    o_bound[...] = chosen * (
        held + jnp.dot(input_step, w[...], precision=PRECISE, preferred_element_type=F32)
    )
    totals = above + group_stats + below
    tops = totals[:, 0:3]
    scale = totals[:, 3:6]
    spot = lax.broadcasted_iota(jnp.int32, (1, 3), 1)
    horizon = sections * n
    entries = jnp.where(spot == 0, ns, jnp.where(spot == 1, ns + nu, nu)).astype(F32)
    o_norm[...] = jnp.sqrt(tops / (scale + floor_share * horizon * entries))

    @pl.when(me > 0)
    def _():
        to_earlier.wait_send()

    @pl.when(me < n - 1)
    def _():
        to_later.wait_send()

    for copy in p_copies + b_copies + f_copies:
        copy.wait_send()

    @pl.when(at_group > 0)
    def _():
        to_before.wait_send()

    @pl.when(at_group < groups - 1)
    def _():
        to_after.wait_send()


def local(n, *args):
    size = 4 if n % 4 == 0 else (2 if n % 2 == 0 else 1)
    sections, ns = args[12].shape
    nu = args[13].shape[1]
    mates = size - 1
    copies = [pltpu.VMEM(x.shape, x.dtype) for x in args]
    message = (8, ns)
    dma = pltpu.SemaphoreType.DMA
    scratch = copies + [
        pltpu.VMEM((sections, ns, ns), F32),
        pltpu.VMEM((sections, ns, ns), F32),
        pltpu.VMEM((size, ns, ns), F32),
        pltpu.VMEM((ns, ns), F32),
        pltpu.VMEM((sections, ns), F32),
        pltpu.VMEM((sections, ns), F32),
        pltpu.VMEM((sections, ns), F32),
        pltpu.VMEM((sections, ns), F32),
        pltpu.VMEM((sections, ns), F32),
        pltpu.VMEM((ns, LANES), F32),
    ] + [pltpu.VMEM(message, F32)] * 4 + [
        pltpu.VMEM((size,) + message, F32),
        pltpu.VMEM((size,) + message, F32),
    ] + [pltpu.VMEM(message, F32)] * 4 + [
        dma((16,)), dma((sections,)), dma((2,)), dma((2,)),
        dma((mates,)), dma((mates,)), dma((mates,)), dma((mates,)), dma((mates,)), dma((mates,)),
        dma((2,)), dma((2,)),
    ]
    outs = [(sections, ns), (sections, nu), (sections, ns), (sections, nu), (1, 3)]
    results = pl.pallas_call(
        functools.partial(kernel, n, size),
        out_shape=[jax.ShapeDtypeStruct(shape, F32) for shape in outs],
        in_specs=[pl.BlockSpec(memory_space=pl.ANY)] * len(args),
        out_specs=[pl.BlockSpec(memory_space=pltpu.VMEM)] * len(outs),
        scratch_shapes=scratch,
        compiler_params=pltpu.CompilerParams(
            collective_id=0, has_side_effects=True, vmem_limit_bytes=60 * 1024 * 1024
        ),
    )(*args)
    return (*results[:4], results[4][0])


def solution(mesh):
    wide = P(("batch", "tm"), None, None)
    flat = P(("batch", "tm"), None)
    in_specs = (wide,) * 6 + (P("batch", None),) + (flat,) * 10
    out_specs = (flat,) * 4 + (P("batch"),)
    return jax.shard_map(
        functools.partial(local, mesh.shape["tm"]),
        mesh=mesh, in_specs=in_specs, out_specs=out_specs, check_vma=False,
    )
```

```python
import functools
import jax
import jax.numpy as jnp
from jax import lax
from jax.experimental import pallas as pl
from jax.experimental.pallas import tpu as pltpu
from jax.sharding import PartitionSpec as P

F32 = jnp.float32
BF16 = jnp.bfloat16
PRECISE = lax.Precision.HIGHEST
MESH = pl.DeviceIdType.MESH
floor_share = 0.001
LANES = 128


def parts_of(x):
    high = x.astype(BF16)
    return high, (x - high.astype(F32)).astype(BF16)


def matmul(a, b):
    ah, al = parts_of(a)
    bh, bl = parts_of(b)
    dot = functools.partial(jnp.dot, preferred_element_type=F32)
    return dot(ah, bh) + (dot(ah, bl) + dot(al, bh))


def turned(x):
    rows, cols = x.shape
    up = -rows % LANES
    side = -cols % LANES
    if up:
        x = jnp.concatenate([x, jnp.zeros((up, cols), F32)], axis=0)
    if side:
        x = jnp.concatenate([x, jnp.zeros((rows + up, side), F32)], axis=1)
    return x.T[:cols, :rows]


def column(row):
    return jnp.broadcast_to(row, (LANES, row.shape[1])).T[:, :1]


def row_of(col):
    return jnp.broadcast_to(col, (col.shape[0], LANES)).T[:1]


def times(matrix, row):
    return jnp.sum(matrix * row, axis=1, keepdims=True)


def times_t(matrix, col):
    return jnp.sum(matrix * col, axis=0, keepdims=True)


def kernel(n, size, *refs):
    (a_hbm, b_hbm, m_hbm, k_hbm, v_hbm, gi_hbm, w_hbm, sw_hbm, sl_hbm, il_hbm, of_hbm, ub_hbm,
     st_hbm, in_hbm, mu_hbm, bm_hbm, ac_hbm,
     o_state, o_input, o_mult, o_bound, o_norm,
     a, b, m, fb, v, gi, w, sw, sl, il, of, ub, st, inp, mu, bm, ac,
     pre, suf, group, whole, sources, pushes, back_local, fwd_local, back,
     cols, fol_in, prd_in, prd_out, fol_out, vec_b, vec_f, ch_b_in, ch_f_in, ch_b_out, ch_f_out,
     load_sem, m_sem, nb_send, nb_recv, p_send, p_recv, b_send, b_recv, f_send, f_recv,
     ch_send, ch_recv) = refs
    me = lax.axis_index("tm")
    place = lax.rem(me, size)
    base = me - place
    at_group = lax.div(me, size)
    groups = n // size
    sections, ns = st.shape
    nu = inp.shape[1]
    half = sections // 2

    order = []
    for i in range(half):
        order += [i, sections - 1 - i]
    for k in order:
        pltpu.make_async_copy(m_hbm.at[k], m.at[k], m_sem.at[k]).start()
    small = [(w_hbm, w), (sw_hbm, sw), (sl_hbm, sl), (il_hbm, il), (of_hbm, of), (ub_hbm, ub),
             (st_hbm, st), (in_hbm, inp), (mu_hbm, mu), (bm_hbm, bm), (ac_hbm, ac)]
    large = [(a_hbm, a), (b_hbm, b), (v_hbm, v), (k_hbm, fb), (gi_hbm, gi)]
    loads = [
        pltpu.make_async_copy(src, dst, load_sem.at[i]) for i, (src, dst) in enumerate(small + large)
    ]
    for load in loads:
        load.start()

    barrier = pltpu.get_barrier_semaphore()
    first_of, last_of = place == 0, place == size - 1
    relations = [
        (jnp.logical_and(first_of, me > 0), me - 1),
        (jnp.logical_and(last_of, me < n - 1), me + 1),
        (at_group > 0, me - size),
        (at_group < groups - 1, me + size),
    ]
    mates = [base + lax.rem(place + j, size) for j in range(1, size)]
    for mate in mates:
        pl.semaphore_signal(barrier, inc=1, device_id={"tm": mate}, device_id_type=MESH)
    for holds, peer in relations:
        @pl.when(holds)
        def _():
            pl.semaphore_signal(barrier, inc=1, device_id={"tm": peer}, device_id_type=MESH)
    def remote(src, dst, send, recv, peer):
        return pltpu.make_async_remote_copy(
            src_ref=src, dst_ref=dst, send_sem=send, recv_sem=recv,
            device_id={"tm": peer}, device_id_type=MESH,
        )

    for load in loads[: len(small)]:
        load.wait()
    to_earlier = remote(fol_out, fol_in, nb_send.at[0], nb_recv.at[0], me - 1)
    to_later = remote(prd_out, prd_in, nb_send.at[1], nb_recv.at[1], me + 1)
    fol_out[...] = jnp.broadcast_to(mu[0:1], fol_out.shape)

    def wait_loop(k):
        pltpu.make_async_copy(m_hbm.at[k], m.at[k], m_sem.at[k]).wait()

    wait_loop(0)
    wait_loop(sections - 1)
    pre[0] = m[0]
    suf[sections - 1] = m[sections - 1]

    def grow(i, waits):
        j = sections - 1 - i
        if waits:
            wait_loop(i)
            wait_loop(j)
        pre[i] = matmul(m[i], pre[i - 1])
        suf[j] = matmul(suf[j + 1], m[j])

    @pl.loop(1, half)
    def _(i):
        grow(i, True)

    product = matmul(suf[half], pre[half - 1])
    suf[0] = product
    group[pl.ds(place, 1)] = product[None]
    peers = size - 1
    for holds, peer in relations:
        peers = peers + jnp.where(holds, 1, 0)
    pl.semaphore_wait(barrier, peers)

    @pl.when(me > 0)
    def _():
        to_earlier.start()

    along = place + 1 - 2 * lax.rem(place, 2)
    across = place + 2 - 4 * lax.div(place, 2)
    far = size - 1 - place
    top, bottom = pl.ds(0, ns // 2), pl.ds(ns // 2, ns // 2)

    def whole_block(slot, j, peer):
        return remote(group.at[slot], group.at[slot], p_send.at[j], p_recv.at[j], base + peer)

    def half_block(slot, rows, j, peer):
        ref = group.at[slot, rows]
        return remote(ref, ref, p_send.at[j], p_recv.at[j], base + peer)

    if size == 4:
        p_copies = [whole_block(place, 0, along), whole_block(place, 1, across)]
    else:
        p_copies = [
            whole_block(place, j, lax.rem(place + j + 1, size)) for j in range(size - 1)
        ]
    for copy in p_copies:
        copy.start()

    for load in loads[len(small):]:
        load.wait()
    lane = lax.broadcasted_iota(jnp.int32, (ns, LANES), 1)
    lane_u = lax.broadcasted_iota(jnp.int32, (nu, LANES), 1)

    inputs_t = turned(inp[...])
    acc = jnp.zeros((ns, LANES), F32)
    for k in range(sections):
        acc = jnp.where(lane == k, times(a[k], st[k:k + 1]), acc)
    predicted = acc.T[:sections]
    rows = [times_t(b[k], inputs_t[:, k:k + 1]) for k in range(sections)]
    predicted = predicted + jnp.concatenate(rows, axis=0)
    prd_out[...] = jnp.broadcast_to(predicted[sections - 1:], prd_out.shape)

    @pl.when(me < n - 1)
    def _():
        to_later.start()

    @pl.loop(half, sections - 1)
    def _(i):
        grow(i, False)

    @pl.when(me < n - 1)
    def _():
        to_earlier.wait_recv()

    @pl.when(me == n - 1)
    def _():
        fol_in[...] = jnp.zeros_like(fol_in)

    following = jnp.concatenate([mu[1:], fol_in[0:1]], axis=0)
    following_t = turned(following)
    grad_input = (
        jnp.dot(inp[...], w[...], precision=PRECISE, preferred_element_type=F32) + il[...] + bm[...]
    )
    acc = jnp.zeros((nu, LANES), F32)
    for k in range(sections):
        acc = jnp.where(lane_u == k, times(b[k], following[k:k + 1]), acc)
    grad_input = grad_input - turned(acc)[:sections]
    grad_input_t = turned(grad_input)
    rows = [times_t(a[k], following_t[:, k:k + 1]) for k in range(sections)]
    grad_state = sw[...] * st[...] + sl[...] + mu[...] - jnp.concatenate(rows, axis=0)

    @pl.when(me > 0)
    def _():
        to_later.wait_recv()

    @pl.when(me == 0)
    def _():
        prd_in[...] = jnp.zeros_like(prd_in)

    previous = jnp.concatenate([prd_in[0:1], predicted[:sections - 1]], axis=0)
    defect = st[...] - previous - of[...]
    defect_t = turned(defect)
    rows = [
        times_t(v[k], defect_t[:, k:k + 1]) + times_t(fb[k], grad_input_t[:, k:k + 1])
        for k in range(sections)
    ]
    sources[...] = jnp.concatenate(rows, axis=0) + grad_state
    slack = bm[...] * (ub[...] - inp[...])

    def total(*xs):
        return sum(
            jnp.sum(jnp.sum(x * x, axis=1, keepdims=True), axis=0, keepdims=True) for x in xs
        )

    sums = [total(defect), total(grad_state, grad_input), total(slack), total(of[...]),
            total(sl[...], il[...]), total(bm[...])]
    line = lax.broadcasted_iota(jnp.int32, (1, ns), 1)
    stats = jnp.zeros((1, ns), F32)
    for i, value in enumerate(sums):
        stats = jnp.where(line == i, value, stats)

    def packed(vector, extra):
        return jnp.concatenate([vector, extra, jnp.zeros((6, ns), F32)], axis=0)

    sources_t = turned(sources[...])
    costate = sources[0:1]
    for k in range(1, sections):
        costate = costate + times_t(pre[k - 1], sources_t[:, k:k + 1])
    vec_b[pl.ds(place, 1)] = packed(costate, stats)[None]
    b_copies = [
        remote(vec_b.at[place], vec_b.at[place], b_send.at[j], b_recv.at[j], mate)
        for j, mate in enumerate(mates)
    ]
    for copy in b_copies:
        copy.start()

    def arrive(buffer, send, recv):
        for j in range(size - 1):
            source = base + lax.rem(place + size - 1 - j, size)
            slot = source - base
            remote(buffer.at[slot], buffer.at[slot], send.at[j], recv.at[j], source).wait_recv()

    if size == 4:
        whole_block(along, 0, along).wait_recv()
        second = half_block(along, top, 2, across)
        second.start()
        whole_block(across, 1, across).wait_recv()
        third = half_block(across, bottom, 3, along)
        third.start()
        p_copies = p_copies + [second, third]

    costate = sources[sections - 1:]
    back_local[sections - 1:] = costate
    for k in range(sections - 2, -1, -1):
        costate = times_t(m[k], column(costate)) + sources[k:k + 1]
        back_local[k:k + 1] = costate

    arrive(vec_b, b_send, b_recv)
    if size == 4:
        half_block(far, top, 2, across).wait_recv()
        half_block(far, bottom, 3, along).wait_recv()
    else:
        arrive(group, p_send, p_recv)
    joined = group[0]
    for e in range(1, size):
        joined = matmul(group[e], joined)
    whole[...] = joined
    group_stats = jnp.sum(vec_b[:, 1, :], axis=0, keepdims=True)

    y = vec_b[size - 1, 0:1]
    for e in range(size - 2, -1, -1):
        y = vec_b[e, 0:1] + times_t(group[e], column(y))
    to_before = remote(ch_b_out, ch_b_in, ch_send.at[0], ch_recv.at[0], me - size)
    to_after = remote(ch_f_out, ch_f_in, ch_send.at[1], ch_recv.at[1], me + size)

    @pl.when(at_group < groups - 1)
    def _():
        to_before.wait_recv()

    @pl.when(at_group == groups - 1)
    def _():
        ch_b_in[...] = jnp.zeros_like(ch_b_in)

    incoming = ch_b_in[0:1]
    above = ch_b_in[1:2]
    ch_b_out[...] = packed(times_t(whole[...], column(incoming)) + y, above + group_stats)

    @pl.when(at_group > 0)
    def _():
        to_before.start()

    for e in range(size - 1, 0, -1):
        new = vec_b[e, 0:1] + times_t(group[e], column(incoming))
        incoming = jnp.where(place < e, new, incoming)

    incoming_c = column(incoming)
    for k in range(sections):
        back[k:k + 1] = times_t(suf[k], incoming_c) + back_local[k:k + 1]
    before = back[...]
    after = jnp.concatenate([before[1:], incoming], axis=0)
    acc = jnp.zeros((nu, LANES), F32)
    for k in range(sections):
        acc = jnp.where(lane_u == k, times(b[k], after[k:k + 1]), acc)
    pulled = turned(acc)[:sections]
    held = grad_input + pulled
    acc = jnp.zeros((nu, LANES), F32)
    for k in range(sections):
        gain = -times(gi[k], held[k:k + 1])
        acc = jnp.where(lane_u == k, gain, acc)
        pushes[k:k + 1] = times_t(b[k], gain)
    forward_gain = turned(acc)[:sections]

    acc = jnp.zeros((ns, ns), F32)
    for k in range(sections):
        drive = -defect[k:k + 1]
        if k:
            drive = drive + pushes[k - 1:k]
        acc = acc + suf[k] * drive
    ended = row_of(jnp.sum(acc, axis=1, keepdims=True)) + pushes[sections - 1:]
    vec_f[pl.ds(place, 1)] = packed(ended, stats)[None]
    f_copies = [
        remote(vec_f.at[place], vec_f.at[place], f_send.at[j], f_recv.at[j], mate)
        for j, mate in enumerate(mates)
    ]
    for copy in f_copies:
        copy.start()

    def forward_alone():
        step = -defect[0:1]
        acc = jnp.where(lane == 0, column(step), 0.0)
        for k in range(1, sections):
            moved = times(m[k - 1], step)
            step = row_of(moved) + pushes[k - 1:k] - defect[k:k + 1]
            acc = jnp.where(lane == k, column(step), acc)
        cols[...] = acc

    @pl.when(at_group > 0)
    def _():
        forward_alone()

    arrive(vec_f, f_send, f_recv)
    y = vec_f[0, 0:1]
    for e in range(1, size):
        y = vec_f[e, 0:1] + row_of(times(group[e], y))

    @pl.when(at_group > 0)
    def _():
        to_after.wait_recv()

    @pl.when(at_group == 0)
    def _():
        ch_f_in[...] = jnp.zeros_like(ch_f_in)

    entering = ch_f_in[0:1]
    below = ch_f_in[1:2]
    ch_f_out[...] = packed(row_of(times(whole[...], entering)) + y, below + group_stats)

    @pl.when(at_group < groups - 1)
    def _():
        to_after.start()

    @pl.when(at_group == 0)
    def _():
        forward_alone()

    for e in range(size - 1):
        new = vec_f[e, 0:1] + row_of(times(group[e], entering))
        entering = jnp.where(place > e, new, entering)

    acc = cols[...] + jnp.where(lane == 0, column(entering), 0.0)
    for k in range(1, sections):
        acc = acc + jnp.where(lane == k, times(pre[k - 1], entering), 0.0)
    state_step = acc.T[:sections]
    o_state[...] = state_step
    moved = acc[:, :sections] - defect_t
    for k in range(sections):
        o_mult[k:k + 1] = times_t(v[k], moved[:, k:k + 1]) + back[k:k + 1]
    acc = jnp.zeros((nu, LANES), F32)
    for k in range(sections):
        acc = jnp.where(lane_u == k, times(fb[k], state_step[k:k + 1]), acc)
    fed = turned(acc)[:sections]
    chosen = ac[...].astype(F32)
    input_step = (1.0 - chosen) * (fed + forward_gain) + chosen * (ub[...] - inp[...])
    o_input[...] = input_step
    o_bound[...] = chosen * (
        held + jnp.dot(input_step, w[...], precision=PRECISE, preferred_element_type=F32)
    )
    totals = above + group_stats + below
    tops = totals[:, 0:3]
    scale = totals[:, 3:6]
    spot = lax.broadcasted_iota(jnp.int32, (1, 3), 1)
    horizon = sections * n
    entries = jnp.where(spot == 0, ns, jnp.where(spot == 1, ns + nu, nu)).astype(F32)
    o_norm[...] = jnp.sqrt(tops / (scale + floor_share * horizon * entries))

    @pl.when(me > 0)
    def _():
        to_earlier.wait_send()

    @pl.when(me < n - 1)
    def _():
        to_later.wait_send()

    for copy in p_copies + b_copies + f_copies:
        copy.wait_send()

    @pl.when(at_group > 0)
    def _():
        to_before.wait_send()

    @pl.when(at_group < groups - 1)
    def _():
        to_after.wait_send()


def local(n, *args):
    size = 4 if n % 4 == 0 else (2 if n % 2 == 0 else 1)
    sections, ns = args[12].shape
    nu = args[13].shape[1]
    mates = size - 1
    copies = [pltpu.VMEM(x.shape, x.dtype) for x in args]
    message = (8, ns)
    dma = pltpu.SemaphoreType.DMA
    scratch = copies + [
        pltpu.VMEM((sections, ns, ns), F32),
        pltpu.VMEM((sections, ns, ns), F32),
        pltpu.VMEM((size, ns, ns), F32),
        pltpu.VMEM((ns, ns), F32),
        pltpu.VMEM((sections, ns), F32),
        pltpu.VMEM((sections, ns), F32),
        pltpu.VMEM((sections, ns), F32),
        pltpu.VMEM((sections, ns), F32),
        pltpu.VMEM((sections, ns), F32),
        pltpu.VMEM((ns, LANES), F32),
    ] + [pltpu.VMEM(message, F32)] * 4 + [
        pltpu.VMEM((size,) + message, F32),
        pltpu.VMEM((size,) + message, F32),
    ] + [pltpu.VMEM(message, F32)] * 4 + [
        dma((16,)), dma((sections,)), dma((2,)), dma((2,)),
        dma((4,)), dma((4,)), dma((mates,)), dma((mates,)), dma((mates,)), dma((mates,)),
        dma((2,)), dma((2,)),
    ]
    outs = [(sections, ns), (sections, nu), (sections, ns), (sections, nu), (1, 3)]
    results = pl.pallas_call(
        functools.partial(kernel, n, size),
        out_shape=[jax.ShapeDtypeStruct(shape, F32) for shape in outs],
        in_specs=[pl.BlockSpec(memory_space=pl.ANY)] * len(args),
        out_specs=[pl.BlockSpec(memory_space=pltpu.VMEM)] * len(outs),
        scratch_shapes=scratch,
        compiler_params=pltpu.CompilerParams(
            collective_id=0, has_side_effects=True, vmem_limit_bytes=60 * 1024 * 1024
        ),
    )(*args)
    return (*results[:4], results[4][0])


def solution(mesh):
    wide = P(("batch", "tm"), None, None)
    flat = P(("batch", "tm"), None)
    in_specs = (wide,) * 6 + (P("batch", None),) + (flat,) * 10
    out_specs = (flat,) * 4 + (P("batch"),)
    return jax.shard_map(
        functools.partial(local, mesh.shape["tm"]),
        mesh=mesh, in_specs=in_specs, out_specs=out_specs, check_vma=False,
    )
```
